32 devices in a mesh: dp: 8 (over z, y), tensor: 4 (over x, core).
Axes of the slice: x: 2, y: 2, z: 4, core: 2. Of those that a mesh axis runs over, the one named last changes fastest.
Arguments:
- clean_latents: bfloat16 [8, 512, 2048], P('dp', 'tensor'), may hold values from -24 to 24
- noise_latents: bfloat16 [8, 512, 2048], P('dp', 'tensor'), may hold values from -24 to 24
- step_index: int32 [8], P('dp'), may hold values from 0 to 999
- labels: int32 [8], P('dp'), may hold values from 0 to 999
- class_shift: bfloat16 [1000, 2048], replicated, may hold values from -6 to 6
- w_qkv: bfloat16 [2048, 3072], P('dp', 'tensor'), may hold values from -0.2 to 0.2
- w_out_t: bfloat16 [2048, 1024], P('dp', 'tensor'), may hold values from -0.1875 to 0.1875
Outputs:
- grad_qkv: float32 [2048, 3072], P('dp', 'tensor')
- grad_out: float32 [2048, 1024], P('dp', 'tensor')
The draws below stay inside these ranges and needn't reach their ends.
All inputs are finite; a program needn't handle non-finite values.
Results may differ from the reference program's by a relative error of at most 0.0075.
Values may be sent and summed in bfloat16 or wider, within the bound.
No kernel may reach another device: no remote copies, remote signals or barrier semaphores. Data moves between devices by JAX's collectives and lax.ppermute only.
A program may use at most 128 MiB of HBM per device.

```python
import math
import jax
import jax.numpy as jnp
from jax import lax

D = 2048
HEADS = 8
HEAD_DIM = 128
CLASSES = 1000
STEPS = 1000
S = 512
LATENTS = 8


weight_edge = 0.19921875


def latent_draw(key, tag):
    folded = jax.random.fold_in(key, tag)
    key_base, key_rough = jax.random.split(folded, 2)
    full_shape = (LATENTS, S, D)
    rising = 0.5 + jnp.arange(S, dtype=jnp.float32) / S
    roughness = jnp.exp(jax.random.uniform(key_rough, (LATENTS, S, 1), jnp.float32, -0.7, 0.7))
    values = jax.random.normal(key_base, full_shape, jnp.float32) * rising[None, :, None] * roughness
    return jnp.clip(values, -24.0, 24.0).astype(jnp.bfloat16)


def draw_clean_latents(key, part):
    return latent_draw(key, 11)


def draw_noise_latents(key, part):
    return latent_draw(key, 23)


def draw_w_qkv(key, part):
    key_base = jax.random.fold_in(jax.random.fold_in(key, 37), 0)
    full_shape = (D, HEADS, 3, HEAD_DIM)
    values = jax.random.normal(key_base, full_shape, jnp.float32) / math.sqrt(D)
    return jnp.clip(values, -weight_edge, weight_edge).reshape(D, HEADS * 3 * HEAD_DIM).astype(jnp.bfloat16)


def touch_ends(array, own_key, smallest, high):
    longest = array.shape.index(max(array.shape))
    spots = []
    for shift in (0, 1):
        where = [jax.random.randint(jax.random.fold_in(own_key, axis), (), 0, length) for axis, length in enumerate(array.shape)]
        where[longest] = (where[longest] + shift) % array.shape[longest]
        spots.append(tuple(where))
    return array.at[spots[0]].set(smallest).at[spots[1]].set(high)


def block_scale(rng, dims, shards, low, high):
    def one(axis_at, shards_of):
        draws = jax.random.uniform(jax.random.fold_in(jax.random.fold_in(rng, 6), axis_at), (shards_of,), jnp.float32, low / len(shards), high / len(shards))
        return jnp.repeat(jnp.exp(draws), dims[axis_at] // shards_of).reshape((-1,) + (1,) * (len(dims) - axis_at - 1))

    level = one(*shards[0])
    for cut in shards[1:]:
        level = level * one(*cut)
    return level


def bell_draw(own_key, shape, width, limit, pieces=(), kind=jnp.bfloat16):
    loudness = block_scale(own_key, shape, pieces, -0.22, 0.18) if pieces else 1.0
    entries = jax.random.normal(own_key, shape, jnp.float32) * width * loudness
    return jnp.minimum(jnp.maximum(entries, -limit), limit).astype(kind)


def setup_inputs(seed: int = 0) -> dict:
    streams_of = jax.random.split(jax.random.key(seed), 8)
    return {
        "clean_latents": draw_clean_latents(jax.random.fold_in(streams_of[7], 71), 0),
        "noise_latents": draw_noise_latents(jax.random.fold_in(streams_of[7], 71), 0),
        "step_index": touch_ends(jax.random.randint(streams_of[2], (LATENTS,), 0, STEPS), jax.random.fold_in(streams_of[2], 1), 0, STEPS - 1).astype(jnp.int32),
        "labels": touch_ends(jax.random.randint(streams_of[3], (LATENTS,), 0, CLASSES), jax.random.fold_in(streams_of[3], 1), 0, CLASSES - 1).astype(jnp.int32),
        "class_shift": bell_draw(streams_of[4], (CLASSES, D), 1.0, 6.0),
        "w_qkv": draw_w_qkv(jax.random.fold_in(streams_of[7], 71), 0),
        "w_out_t": bell_draw(streams_of[6], (D, HEADS * HEAD_DIM), (HEADS * HEAD_DIM) ** -0.5, 0.1875, ((0, 8), (1, 4))),
    }


norm_eps = 1e-06
target_floor = 0.1

def time_terms(step_index, model_width):
    step_times = 1.4 * (step_index.astype(jnp.float32) + 0.5) / STEPS
    feature_ids = jnp.arange(model_width, dtype=jnp.float32)
    frequency = jnp.exp(-math.log(100.0) * feature_ids / model_width)
    phases = step_times[:, None] * frequency[None, :] + feature_ids[None, :]
    return (step_times, 0.5 * jnp.sin(phases), 0.5 * frequency[None, :] * jnp.cos(phases))

def trig_path(clean_part, noise_part, step_times):
    cos_t = jnp.cos(step_times)[:, None, None]
    sin_t = jnp.sin(step_times)[:, None, None]
    clean_wide = clean_part.astype(jnp.float32)
    noise_wide = noise_part.astype(jnp.float32)
    return (cos_t * clean_wide + sin_t * noise_wide, cos_t * noise_wide - sin_t * clean_wide)

def modulate(noisy, velocity, amplitude, amp_rate, class_offset):
    inverse = lax.rsqrt(lax.optimization_barrier(jnp.mean(noisy * noisy, axis=-1, keepdims=True)) + norm_eps)
    normed = noisy * inverse
    normed_rate = velocity * inverse - noisy * inverse ** 3 * lax.optimization_barrier(jnp.mean(noisy * velocity, axis=-1, keepdims=True))
    scale_up = 1.0 + amplitude[:, None, :]
    mixed = normed * scale_up + class_offset[:, None, :]
    mixed_rate = normed_rate * scale_up + normed * amp_rate[:, None, :]
    return (mixed.astype(jnp.bfloat16), mixed_rate.astype(jnp.bfloat16))

def target_of(noisy, velocity, proj, proj_rate, step_times):
    cos_t = jnp.cos(step_times)[:, None, None]
    sin_t = jnp.sin(step_times)[:, None, None]
    model_out = noisy + proj
    model_rate = velocity + proj_rate
    return -(cos_t * cos_t) * (model_out - velocity) - cos_t * sin_t * (noisy + model_rate)

def wide_einsum(form, left_part, right_part):
    return jnp.einsum(form, left_part.astype(jnp.float32), right_part.astype(jnp.float32))

def attend(projected, projected_rate, score_scale):
    query_part = projected[:, :, :, 0, :]
    key_part = projected[:, :, :, 1, :]
    value_part = projected[:, :, :, 2, :]
    query_rate = projected_rate[:, :, :, 0, :]
    key_rate = projected_rate[:, :, :, 1, :]
    value_rate = projected_rate[:, :, :, 2, :]
    scores = wide_einsum('lqhd,lkhd->lhqk', query_part, key_part) * score_scale
    score_rate = (wide_einsum('lqhd,lkhd->lhqk', query_rate, key_part) + wide_einsum('lqhd,lkhd->lhqk', query_part, key_rate)) * score_scale
    attn_probs = jax.nn.softmax(scores, axis=-1)
    probs_low = attn_probs.astype(jnp.bfloat16)
    prob_rate = attn_probs * (score_rate - lax.optimization_barrier(jnp.sum(attn_probs * score_rate, axis=-1, keepdims=True)))
    prob_rate_low = prob_rate.astype(jnp.bfloat16)
    attn_out = wide_einsum('lhqk,lkhd->lqhd', probs_low, value_part)
    attn_rate = wide_einsum('lhqk,lkhd->lqhd', prob_rate_low, value_part) + wide_einsum('lhqk,lkhd->lqhd', probs_low, value_rate)
    return (attn_probs, probs_low, attn_out.astype(jnp.bfloat16), attn_rate.astype(jnp.bfloat16))

def attend_back(attn_grad, attn_probs, probs_low, projected, score_scale):
    query_part = projected[:, :, :, 0, :]
    key_part = projected[:, :, :, 1, :]
    value_part = projected[:, :, :, 2, :]
    prob_grad = wide_einsum('lqhd,lkhd->lhqk', attn_grad, value_part)
    value_grad = wide_einsum('lhqk,lqhd->lkhd', probs_low, attn_grad)
    score_grad = (attn_probs * (prob_grad - lax.optimization_barrier(jnp.sum(attn_probs * prob_grad, axis=-1, keepdims=True))) * score_scale).astype(jnp.bfloat16)
    query_grad = wide_einsum('lhqk,lkhd->lqhd', score_grad, key_part)
    key_grad = wide_einsum('lhqk,lqhd->lkhd', score_grad, query_part)
    return jnp.stack([query_grad, key_grad, value_grad], axis=3).astype(jnp.bfloat16)

def reference(clean_latents, noise_latents, step_index, labels, class_shift, w_qkv, w_out_t):
    loss_scale = 1.0 / math.sqrt(LATENTS * S)
    score_scale = 1.0 / math.sqrt(HEAD_DIM)
    step_times, amplitude, amp_rate = time_terms(step_index, D)
    class_offset = class_shift[labels].astype(jnp.float32)

    def per_latent(totals, inputs_one):
        grad_in_sum, grad_out_sum = totals
        clean_one, noise_one, time_one, amp_one, rate_one, offset_one = inputs_one
        noisy, velocity = trig_path(clean_one[None], noise_one[None], time_one[None])
        mixed, mixed_rate = modulate(noisy, velocity, amp_one[None], rate_one[None], offset_one[None])
        mixed_rows = mixed.reshape(S, D)
        rate_rows = mixed_rate.reshape(S, D)
        projected = jnp.dot(mixed_rows, w_qkv, preferred_element_type=jnp.float32).astype(jnp.bfloat16).reshape(1, S, HEADS, 3, HEAD_DIM)
        projected_rate = jnp.dot(rate_rows, w_qkv, preferred_element_type=jnp.float32).astype(jnp.bfloat16).reshape(1, S, HEADS, 3, HEAD_DIM)
        attn_probs, probs_low, attn_out, attn_rate = attend(projected, projected_rate, score_scale)
        attn_rows = attn_out.reshape(S, HEADS * HEAD_DIM)
        attn_rate_rows = attn_rate.reshape(S, HEADS * HEAD_DIM)
        proj = jnp.dot(attn_rows, w_out_t.T, preferred_element_type=jnp.float32).reshape(1, S, D)
        proj_rate = jnp.dot(attn_rate_rows, w_out_t.T, preferred_element_type=jnp.float32).reshape(1, S, D)
        target = target_of(noisy, velocity, proj, proj_rate, time_one[None])
        spread = jnp.sqrt(jnp.mean(target * target))
        cotangent = (-(target / (spread + target_floor)) * loss_scale).astype(jnp.bfloat16).reshape(S, D)
        grad_out_sum = grad_out_sum + jnp.dot(cotangent.T, attn_rows, preferred_element_type=jnp.float32)
        attn_grad = jnp.dot(cotangent, w_out_t, preferred_element_type=jnp.float32).astype(jnp.bfloat16).reshape(1, S, HEADS, HEAD_DIM)
        qkv_grad = attend_back(attn_grad, attn_probs, probs_low, projected, score_scale).reshape(S, HEADS * 3 * HEAD_DIM)
        grad_in_sum = grad_in_sum + jnp.dot(mixed_rows.T, qkv_grad, preferred_element_type=jnp.float32)
        return ((grad_in_sum, grad_out_sum), None)
    zero_grads = (jnp.zeros((D, HEADS * 3 * HEAD_DIM), jnp.float32), jnp.zeros((D, HEADS * HEAD_DIM), jnp.float32))
    (grad_qkv, grad_out), _ = lax.scan(per_latent, zero_grads, (clean_latents, noise_latents, step_times, amplitude, amp_rate, class_offset))
    return (grad_qkv, grad_out)
```

```python
import math

import jax
import jax.numpy as jnp
from jax import lax
from jax.sharding import PartitionSpec as P

HEAD_DIM = 128
STEPS = 1000


norm_eps = 1e-06
target_floor = 0.1


def time_terms(step_index, model_width):
    step_times = 1.4 * (step_index.astype(jnp.float32) + 0.5) / STEPS
    feature_ids = jnp.arange(model_width, dtype=jnp.float32)
    frequency = jnp.exp(-math.log(100.0) * feature_ids / model_width)
    phases = step_times[:, None] * frequency[None, :] + feature_ids[None, :]
    return (step_times, 0.5 * jnp.sin(phases), 0.5 * frequency[None, :] * jnp.cos(phases))


def trig_path(clean_part, noise_part, step_times):
    cos_t = jnp.cos(step_times)[:, None, None]
    sin_t = jnp.sin(step_times)[:, None, None]
    clean_wide = clean_part.astype(jnp.float32)
    noise_wide = noise_part.astype(jnp.float32)
    return (cos_t * clean_wide + sin_t * noise_wide, cos_t * noise_wide - sin_t * clean_wide)


def modulate(noisy, velocity, amplitude, amp_rate, class_offset):
    inverse = lax.rsqrt(jnp.mean(noisy * noisy, axis=-1, keepdims=True) + norm_eps)
    normed = noisy * inverse
    normed_rate = velocity * inverse - noisy * inverse**3 * jnp.mean(
        noisy * velocity, axis=-1, keepdims=True
    )
    scale_up = 1.0 + amplitude[:, None, :]
    mixed = normed * scale_up + class_offset[:, None, :]
    mixed_rate = normed_rate * scale_up + normed * amp_rate[:, None, :]
    return (mixed.astype(jnp.bfloat16), mixed_rate.astype(jnp.bfloat16))


def low_einsum(form, left_part, right_part):
    return jnp.einsum(form, left_part, right_part, preferred_element_type=jnp.float32)


def attend(projected, projected_rate, score_scale):
    query_part = projected[:, :, :, 0, :]
    key_part = projected[:, :, :, 1, :]
    value_part = projected[:, :, :, 2, :]
    query_rate = projected_rate[:, :, :, 0, :]
    key_rate = projected_rate[:, :, :, 1, :]
    value_rate = projected_rate[:, :, :, 2, :]
    scores = low_einsum("lqhd,lkhd->lhqk", query_part, key_part) * score_scale
    score_rate = (
        low_einsum("lqhd,lkhd->lhqk", query_rate, key_part)
        + low_einsum("lqhd,lkhd->lhqk", query_part, key_rate)
    ) * score_scale
    attn_probs = jax.nn.softmax(scores, axis=-1)
    probs_low = attn_probs.astype(jnp.bfloat16)
    prob_rate = attn_probs * (score_rate - jnp.sum(attn_probs * score_rate, axis=-1, keepdims=True))
    prob_rate_low = prob_rate.astype(jnp.bfloat16)
    attn_out = low_einsum("lhqk,lkhd->lqhd", probs_low, value_part)
    attn_rate = low_einsum("lhqk,lkhd->lqhd", prob_rate_low, value_part) + low_einsum(
        "lhqk,lkhd->lqhd", probs_low, value_rate
    )
    return (attn_probs, probs_low, attn_out, attn_rate)


def attend_back(attn_grad, attn_probs, probs_low, projected, score_scale):
    query_part = projected[:, :, :, 0, :]
    key_part = projected[:, :, :, 1, :]
    value_part = projected[:, :, :, 2, :]
    prob_grad = low_einsum("lqhd,lkhd->lhqk", attn_grad, value_part)
    value_grad = low_einsum("lhqk,lqhd->lkhd", probs_low, attn_grad)
    score_grad = (
        attn_probs
        * (prob_grad - jnp.sum(attn_probs * prob_grad, axis=-1, keepdims=True))
        * score_scale
    ).astype(jnp.bfloat16)
    query_grad = low_einsum("lhqk,lkhd->lqhd", score_grad, key_part)
    key_grad = low_einsum("lhqk,lqhd->lkhd", score_grad, query_part)
    return jnp.stack([query_grad, key_grad, value_grad], axis=3).astype(jnp.bfloat16)


def shift(part, axis_name, pairs):
    return lax.ppermute(part, axis_name, pairs)


def swap_pairs(size, bit):
    return [(i, i ^ bit) for i in range(size)]


def token_gather(own):
    size = lax.axis_size("tensor")
    far = shift(own, "tensor", swap_pairs(size, 2))
    near = shift(own, "tensor", swap_pairs(size, 1))
    cross = shift(far, "tensor", swap_pairs(size, 1))
    return jnp.concatenate([own, near, far, cross], axis=1)


def token_scatter(near_part, far_part):
    size = lax.axis_size("tensor")
    half = near_part.shape[1] // 2
    low = jnp.bfloat16
    far_got = shift(far_part[:, half:].astype(low), "tensor", swap_pairs(size, 1))
    far_sum = (far_part[:, :half] + far_got).astype(low)
    own_far = shift(far_sum, "tensor", swap_pairs(size, 2))
    near_got = shift(near_part[:, half:].astype(low), "tensor", swap_pairs(size, 1))
    return near_part[:, :half] + near_got + own_far


def line_orders(length):
    return [
        sorted(range(length), key=lambda d, p=p: (abs(d - p), d > p)) for p in range(length)
    ]


def pick(place, choices):
    named = [c for c in choices if c is not None]
    result = named[-1]
    for p in range(len(choices) - 1, -1, -1):
        if choices[p] is not None and choices[p] is not result:
            result = jnp.where(place == p, choices[p], result)
    return result


def line_pairs(length, step, places):
    return [(2 * p + q, 2 * (p + step) + q) for p in places for q in (0, 1)]


def gather_rows(part):
    size = lax.axis_size("dp")
    length = size // 2
    place = lax.axis_index("dp") // 2
    side = lax.axis_index("dp") % 2
    rows = part.shape[0]
    orders = line_orders(length)
    table = jnp.array(orders, dtype=jnp.int32)
    from_below, from_above = [part], [part]
    for s in range(1, length):
        from_below.append(shift(from_below[-1], "dp", line_pairs(length, 1, range(s - 1, length - 1))))
        from_above.append(shift(from_above[-1], "dp", line_pairs(length, -1, range(1, length - s + 1))))
    whole = jnp.zeros((size * rows, part.shape[1]), part.dtype)
    others = []
    for k in range(length):
        choices = []
        for p in range(length):
            d = orders[p][k]
            choices.append(from_below[p - d] if d <= p else from_above[d - p])
        item = part if k == 0 else pick(place, choices)
        other = shift(item, "dp", swap_pairs(size, 1))
        others.append(other)
        at = table[place, k] * 2
        whole = lax.dynamic_update_slice(whole, item, ((at + side) * rows, 0))
        whole = lax.dynamic_update_slice(whole, other, ((at + 1 - side) * rows, 0))
    return whole, others


def scatter_rows(full):
    size = lax.axis_size("dp")
    length = size // 2
    place = lax.axis_index("dp") // 2
    side = lax.axis_index("dp") % 2
    rows = full.shape[0] // size
    low = jnp.bfloat16
    orders = line_orders(length)
    table = jnp.array(orders, dtype=jnp.int32)
    sums = [None] * length
    for k in range(length - 1, -1, -1):
        at = table[place, k] * 2
        send = lax.dynamic_slice_in_dim(full, (at + 1 - side) * rows, rows, axis=0).astype(low)
        got = shift(send, "dp", swap_pairs(size, 1))
        sums[k] = lax.dynamic_slice_in_dim(full, (at + side) * rows, rows, axis=0) + got
    total = sums[0]
    for step in (1, -1):
        got = None
        for s in range(length - 1, 0, -1):
            senders = [p for p in range(length) if 0 <= p + step * s < length]
            choices = [
                sums[orders[p].index(p + step * s)] if p in senders else None for p in range(length)
            ]
            send = pick(place, choices)
            send = send if got is None else send + got
            got = shift(send.astype(low), "dp", line_pairs(length, step, senders))
        total = total + got
    return total


def local(clean_latents, noise_latents, step_index, labels, class_shift, w_qkv, w_out_t):
    latent_count, part_len, model_width = clean_latents.shape
    head_cols = w_out_t.shape[1]
    heads_here = head_cols // HEAD_DIM
    score_scale = 1.0 / math.sqrt(HEAD_DIM)
    dp_size = lax.axis_size("dp")
    lined = dp_size % 2 == 0 and 4 <= dp_size <= 8
    grouped = lax.axis_size("tensor") == 4
    step_times, amplitude, amp_rate = time_terms(step_index, model_width)
    class_offset = jnp.concatenate(
        [lax.dynamic_slice_in_dim(class_shift, labels[i], 1, axis=0) for i in range(latent_count)]
    ).astype(jnp.float32)
    if lined:
        qkv_all, arrived = gather_rows(w_qkv)
        out_own, _ = lax.optimization_barrier((w_out_t, arrived[-2]))
        out_all, _ = gather_rows(out_own)
    else:
        qkv_all = lax.all_gather(w_qkv, "dp", axis=0, tiled=True)
        out_all = lax.all_gather(w_out_t, "dp", axis=0, tiled=True)
    noisy, velocity = trig_path(clean_latents, noise_latents, step_times)
    mixed_own, rate_own = modulate(noisy, velocity, amplitude, amp_rate, class_offset)
    if grouped:
        mixed, mixed_rate = token_gather(mixed_own), token_gather(rate_own)
    else:
        mixed = lax.all_gather(mixed_own, "tensor", axis=1, tiled=True)
        mixed_rate = lax.all_gather(rate_own, "tensor", axis=1, tiled=True)
    seq_len = mixed.shape[1]
    row_count = latent_count * seq_len
    loss_scale = 1.0 / math.sqrt(dp_size * latent_count * seq_len)
    mixed_rows = mixed.reshape(row_count, model_width)
    rate_rows = mixed_rate.reshape(row_count, model_width)
    projected = jnp.dot(mixed_rows, qkv_all, preferred_element_type=jnp.float32)
    projected_rate = jnp.dot(rate_rows, qkv_all, preferred_element_type=jnp.float32)
    projected = projected.astype(jnp.bfloat16).reshape(
        latent_count, seq_len, heads_here, 3, HEAD_DIM
    )
    projected_rate = projected_rate.astype(jnp.bfloat16).reshape(
        latent_count, seq_len, heads_here, 3, HEAD_DIM
    )
    attn_probs, probs_low, attn_out, attn_rate = attend(projected, projected_rate, score_scale)
    cos_t = jnp.cos(step_times)[:, None, None]
    sin_t = jnp.sin(step_times)[:, None, None]
    attn_flat = attn_out.reshape(latent_count, seq_len, head_cols)
    rate_flat = attn_rate.reshape(latent_count, seq_len, head_cols)
    attn_low = attn_flat.astype(jnp.bfloat16)
    blend = (-(cos_t * cos_t) * attn_flat - cos_t * sin_t * rate_flat).astype(jnp.bfloat16)
    if grouped:
        half = seq_len // 2
        far_sums = low_einsum("lsk,dk->lsd", blend[:, half:], out_all)
        near_sums = low_einsum("lsk,dk->lsd", blend[:, :half], out_all)
        own_sums = token_scatter(near_sums, far_sums)
    else:
        head_sums = low_einsum("lsk,dk->lsd", blend, out_all)
        own_sums = lax.psum_scatter(head_sums, "tensor", scatter_dimension=1, tiled=True)
    target = -(cos_t * cos_t) * (noisy - velocity) - cos_t * sin_t * (noisy + velocity) + own_sums
    target_low = target.astype(jnp.bfloat16)
    squares = jnp.sum(target * target, axis=(1, 2))
    if grouped:
        target_all = token_gather(target_low)
        squares = squares + shift(squares, "tensor", swap_pairs(4, 1))
        squares = squares + shift(squares, "tensor", swap_pairs(4, 2))
    else:
        target_all = lax.all_gather(target_low, "tensor", axis=1, tiled=True)
        squares = lax.psum(squares, "tensor")
    spread = jnp.sqrt(squares / (seq_len * model_width))
    grad_scale = (-loss_scale / (spread + target_floor))[:, None, None]
    out_partial = jnp.sum(grad_scale * low_einsum("lsi,lsj->lij", target_all, attn_low), axis=0)
    attn_grad = (grad_scale * low_einsum("lsi,ij->lsj", target_all, out_all)).astype(jnp.bfloat16)
    attn_grad = attn_grad.reshape(latent_count, seq_len, heads_here, HEAD_DIM)
    qkv_grad = attend_back(attn_grad, attn_probs, probs_low, projected, score_scale).reshape(
        row_count, 3 * head_cols
    )
    in_partial = lax.dot_general(
        mixed_rows, qkv_grad, (((0,), (0,)), ((), ())), preferred_element_type=jnp.float32
    )
    if lined:
        return (scatter_rows(in_partial), scatter_rows(out_partial))
    return (
        lax.psum_scatter(in_partial, "dp", scatter_dimension=0, tiled=True),
        lax.psum_scatter(out_partial, "dp", scatter_dimension=0, tiled=True),
    )


def solution(mesh):
    in_specs = (
        P("dp", "tensor", None),
        P("dp", "tensor", None),
        P("dp"),
        P("dp"),
        P(),
        P("dp", "tensor"),
        P("dp", "tensor"),
    )
    out_specs = (P("dp", "tensor"), P("dp", "tensor"))
    return jax.shard_map(local, mesh=mesh, in_specs=in_specs, out_specs=out_specs, check_vma=False)
```

```python
import math

import jax
import jax.numpy as jnp
from jax import lax
from jax.sharding import PartitionSpec as P

HEAD_DIM = 128
STEPS = 1000


norm_eps = 1e-06
target_floor = 0.1


def time_terms(step_index, model_width):
    step_times = 1.4 * (step_index.astype(jnp.float32) + 0.5) / STEPS
    feature_ids = jnp.arange(model_width, dtype=jnp.float32)
    frequency = jnp.exp(-math.log(100.0) * feature_ids / model_width)
    phases = step_times[:, None] * frequency[None, :] + feature_ids[None, :]
    return (step_times, 0.5 * jnp.sin(phases), 0.5 * frequency[None, :] * jnp.cos(phases))


def trig_path(clean_part, noise_part, step_times):
    cos_t = jnp.cos(step_times)[:, None, None]
    sin_t = jnp.sin(step_times)[:, None, None]
    clean_wide = clean_part.astype(jnp.float32)
    noise_wide = noise_part.astype(jnp.float32)
    return (cos_t * clean_wide + sin_t * noise_wide, cos_t * noise_wide - sin_t * clean_wide)


def modulate(noisy, velocity, amplitude, amp_rate, class_offset):
    inverse = lax.rsqrt(jnp.mean(noisy * noisy, axis=-1, keepdims=True) + norm_eps)
    normed = noisy * inverse
    normed_rate = velocity * inverse - noisy * inverse**3 * jnp.mean(
        noisy * velocity, axis=-1, keepdims=True
    )
    scale_up = 1.0 + amplitude[:, None, :]
    mixed = normed * scale_up + class_offset[:, None, :]
    mixed_rate = normed_rate * scale_up + normed * amp_rate[:, None, :]
    return (mixed.astype(jnp.bfloat16), mixed_rate.astype(jnp.bfloat16))


def low_einsum(form, left_part, right_part):
    return jnp.einsum(form, left_part, right_part, preferred_element_type=jnp.float32)


def attend(projected, projected_rate, score_scale):
    query_part = projected[:, :, :, 0, :]
    key_part = projected[:, :, :, 1, :]
    value_part = projected[:, :, :, 2, :]
    query_rate = projected_rate[:, :, :, 0, :]
    key_rate = projected_rate[:, :, :, 1, :]
    value_rate = projected_rate[:, :, :, 2, :]
    scores = low_einsum("lqhd,lkhd->lhqk", query_part, key_part) * score_scale
    score_rate = (
        low_einsum("lqhd,lkhd->lhqk", query_rate, key_part)
        + low_einsum("lqhd,lkhd->lhqk", query_part, key_rate)
    ) * score_scale
    attn_probs = jax.nn.softmax(scores, axis=-1)
    probs_low = attn_probs.astype(jnp.bfloat16)
    prob_rate = attn_probs * (score_rate - jnp.sum(attn_probs * score_rate, axis=-1, keepdims=True))
    prob_rate_low = prob_rate.astype(jnp.bfloat16)
    attn_out = low_einsum("lhqk,lkhd->lqhd", probs_low, value_part)
    attn_rate = low_einsum("lhqk,lkhd->lqhd", prob_rate_low, value_part) + low_einsum(
        "lhqk,lkhd->lqhd", probs_low, value_rate
    )
    return (attn_probs, probs_low, attn_out, attn_rate)


def attend_back(attn_grad, attn_probs, probs_low, projected, score_scale):
    query_part = projected[:, :, :, 0, :]
    key_part = projected[:, :, :, 1, :]
    value_part = projected[:, :, :, 2, :]
    prob_grad = low_einsum("lqhd,lkhd->lhqk", attn_grad, value_part)
    value_grad = low_einsum("lhqk,lqhd->lkhd", probs_low, attn_grad)
    score_grad = (
        attn_probs
        * (prob_grad - jnp.sum(attn_probs * prob_grad, axis=-1, keepdims=True))
        * score_scale
    ).astype(jnp.bfloat16)
    query_grad = low_einsum("lhqk,lkhd->lqhd", score_grad, key_part)
    key_grad = low_einsum("lhqk,lqhd->lkhd", score_grad, query_part)
    return jnp.stack([query_grad, key_grad, value_grad], axis=3)


def shift(part, axis_name, pairs):
    return lax.ppermute(part, axis_name, pairs)


def swap_pairs(size, bit):
    return [(i, i ^ bit) for i in range(size)]


def token_gather(own):
    size = lax.axis_size("tensor")
    blocks = [own] * size
    for b in sorted(range(1, size), key=lambda b: b % 2 and b > 1):
        base, bit = (blocks[b - 1], 1) if b % 2 else (own, b)
        blocks[b] = shift(base, "tensor", swap_pairs(size, bit))
    return blocks


def token_exchange(blocks):
    size = lax.axis_size("tensor")
    return [blocks[0]] + [
        shift(blocks[b], "tensor", swap_pairs(size, b)) for b in range(1, size)
    ]


def line_orders(length):
    return [
        sorted(range(length), key=lambda d, p=p: (abs(d - p), d > p)) for p in range(length)
    ]


def pick(place, choices):
    named = [c for c in choices if c is not None]
    result = named[-1]
    for p in range(len(choices) - 1, -1, -1):
        if choices[p] is not None and choices[p] is not result:
            result = jnp.where(place == p, choices[p], result)
    return result


def line_pairs(length, step, places):
    return [(2 * p + q, 2 * (p + step) + q) for p in places for q in (0, 1)]


def gather_rows(part, guards=()):
    size = lax.axis_size("dp")
    length = size // 2
    place = lax.axis_index("dp") // 2
    side = lax.axis_index("dp") % 2
    rows = part.shape[0]
    orders = line_orders(length)
    table = jnp.array(orders, dtype=jnp.int32)
    from_below, from_above = [part], [part]
    for s in range(1, length):
        from_below.append(shift(from_below[-1], "dp", line_pairs(length, 1, range(s - 1, length - 1))))
        from_above.append(shift(from_above[-1], "dp", line_pairs(length, -1, range(1, length - s + 1))))
        if s <= len(guards):
            from_below[s], from_above[s], _ = lax.optimization_barrier(
                (from_below[s], from_above[s], guards[s - 1])
            )
    whole = jnp.zeros((size * rows, part.shape[1]), part.dtype)
    for k in range(length):
        choices = []
        for p in range(length):
            d = orders[p][k]
            choices.append(from_below[p - d] if d <= p else from_above[d - p])
        item = part if k == 0 else pick(place, choices)
        other = shift(item, "dp", swap_pairs(size, 1))
        at = table[place, k] * 2
        whole = lax.dynamic_update_slice(whole, item, ((at + side) * rows, 0))
        whole = lax.dynamic_update_slice(whole, other, ((at + 1 - side) * rows, 0))
    return whole, (from_below[-1], from_above[-1])


def scatter_rows(full):
    size = lax.axis_size("dp")
    length = size // 2
    place = lax.axis_index("dp") // 2
    side = lax.axis_index("dp") % 2
    rows = full.shape[0] // size
    low = jnp.bfloat16
    orders = line_orders(length)
    table = jnp.array(orders, dtype=jnp.int32)
    sums = [None] * length
    first = None
    for k in range(length - 1, -1, -1):
        at = table[place, k] * 2
        send = lax.dynamic_slice_in_dim(full, (at + 1 - side) * rows, rows, axis=0).astype(low)
        got = shift(send, "dp", swap_pairs(size, 1))
        first = got if first is None else first
        sums[k] = lax.dynamic_slice_in_dim(full, (at + side) * rows, rows, axis=0) + got
    total = sums[0]
    for step in (1, -1):
        got = None
        for s in range(length - 1, 0, -1):
            senders = [p for p in range(length) if 0 <= p + step * s < length]
            choices = [
                sums[orders[p].index(p + step * s)] if p in senders else None for p in range(length)
            ]
            send = pick(place, choices)
            send = send if got is None else send + got
            got = shift(send.astype(low), "dp", line_pairs(length, step, senders))
        total = total + got
    return total, first


def local(clean_latents, noise_latents, step_index, labels, class_shift, w_qkv, w_out_t):
    latent_count, part_len, model_width = clean_latents.shape
    head_cols = w_out_t.shape[1]
    heads_here = head_cols // HEAD_DIM
    score_scale = 1.0 / math.sqrt(HEAD_DIM)
    dp_size = lax.axis_size("dp")
    lined = dp_size % 2 == 0 and 4 <= dp_size <= 8
    step_times, amplitude, amp_rate = time_terms(step_index, model_width)
    class_offset = jnp.concatenate(
        [lax.dynamic_slice_in_dim(class_shift, labels[i], 1, axis=0) for i in range(latent_count)]
    ).astype(jnp.float32)
    noisy, velocity = trig_path(clean_latents, noise_latents, step_times)
    mixed_own, rate_own = modulate(noisy, velocity, amplitude, amp_rate, class_offset)
    mixed_blocks, rate_blocks = token_gather(mixed_own), token_gather(rate_own)
    mixed = jnp.concatenate(mixed_blocks, axis=1)
    mixed_rate = jnp.concatenate(rate_blocks, axis=1)
    if lined:
        qkv_all, arrived = gather_rows(w_qkv, ((mixed_own, rate_own), mixed_blocks[-1]))
        out_own, _ = lax.optimization_barrier((w_out_t, arrived))
        out_all, _ = gather_rows(out_own)
    else:
        qkv_all = lax.all_gather(w_qkv, "dp", axis=0, tiled=True)
        out_all = lax.all_gather(w_out_t, "dp", axis=0, tiled=True)
    out_blocks = token_gather(out_all)
    seq_len = mixed.shape[1]
    row_count = latent_count * seq_len
    loss_scale = 1.0 / math.sqrt(dp_size * latent_count * seq_len)
    mixed_rows = mixed.reshape(row_count, model_width)
    rate_rows = mixed_rate.reshape(row_count, model_width)
    projected = jnp.dot(mixed_rows, qkv_all, preferred_element_type=jnp.float32)
    projected_rate = jnp.dot(rate_rows, qkv_all, preferred_element_type=jnp.float32)
    projected = projected.astype(jnp.bfloat16).reshape(
        latent_count, seq_len, heads_here, 3, HEAD_DIM
    )
    projected_rate = projected_rate.astype(jnp.bfloat16).reshape(
        latent_count, seq_len, heads_here, 3, HEAD_DIM
    )
    attn_probs, probs_low, attn_out, attn_rate = attend(projected, projected_rate, score_scale)
    cos_t = jnp.cos(step_times)[:, None, None]
    sin_t = jnp.sin(step_times)[:, None, None]
    attn_flat = attn_out.reshape(latent_count, seq_len, head_cols)
    rate_flat = attn_rate.reshape(latent_count, seq_len, head_cols)
    attn_low = attn_flat.astype(jnp.bfloat16)
    blend = (-(cos_t * cos_t) * attn_flat - cos_t * sin_t * rate_flat).astype(jnp.bfloat16)
    blend_own = token_exchange(jnp.split(blend, seq_len // part_len, axis=1))
    head_sums = sum(low_einsum("lsk,dk->lsd", b, w) for b, w in zip(blend_own, out_blocks))
    target = -(cos_t * cos_t) * (noisy - velocity) - cos_t * sin_t * (noisy + velocity) + head_sums
    target_low = target.astype(jnp.bfloat16)
    attn_grad = token_exchange(
        [low_einsum("lsi,ij->lsj", target_low, w).astype(jnp.bfloat16) for w in out_blocks]
    )
    attn_grad = jnp.concatenate(attn_grad, axis=1).reshape(
        latent_count, seq_len, heads_here, HEAD_DIM
    )
    squares = jnp.sum(target * target, axis=(1, 2))
    bit = 1
    while bit * part_len < seq_len:
        squares = squares + shift(squares, "tensor", swap_pairs(seq_len // part_len, bit))
        bit *= 2
    spread = jnp.sqrt(squares / (seq_len * model_width))
    grad_scale = (-loss_scale / (spread + target_floor))[:, None, None]
    target_all = jnp.concatenate(token_gather(target_low), axis=1)
    out_partial = jnp.sum(grad_scale * low_einsum("lsi,lsj->lij", target_all, attn_low), axis=0)
    qkv_grad = attend_back(attn_grad, attn_probs, probs_low, projected, score_scale)
    qkv_grad = (grad_scale * qkv_grad.reshape(latent_count, seq_len, 3 * head_cols)).astype(
        jnp.bfloat16
    )
    if lined:
        grad_out, first = scatter_rows(out_partial)
        qkv_grad, _ = lax.optimization_barrier((qkv_grad, first))
    in_partial = lax.dot_general(
        mixed_rows,
        qkv_grad.reshape(row_count, 3 * head_cols),
        (((0,), (0,)), ((), ())),
        preferred_element_type=jnp.float32,
    )
    if lined:
        return (scatter_rows(in_partial)[0], grad_out)
    return (
        lax.psum_scatter(in_partial, "dp", scatter_dimension=0, tiled=True),
        lax.psum_scatter(out_partial, "dp", scatter_dimension=0, tiled=True),
    )


def solution(mesh):
    in_specs = (
        P("dp", "tensor", None),
        P("dp", "tensor", None),
        P("dp"),
        P("dp"),
        P(),
        P("dp", "tensor"),
        P("dp", "tensor"),
    )
    out_specs = (P("dp", "tensor"), P("dp", "tensor"))
    return jax.shard_map(local, mesh=mesh, in_specs=in_specs, out_specs=out_specs, check_vma=False)
```
